128 devices in a mesh: fsdp: 32 (over y, z_lo, x), tp: 4 (over z_hi, core).
Axes of the slice: x: 4, y: 4, z: 4 (z_hi: 2, z_lo: 2; z = z_hi * 2 + z_lo), core: 2. Of those that a mesh axis runs over, the one named last changes fastest.
Arguments:
- partials: bfloat16 [32, 2, 5120, 1024], P('fsdp', None, None, 'tp'), may hold values from -6 to 6
- token_counts: int32 [32], P('fsdp'), may hold values from 100 to 599
- owner_map: int32 [2, 4], replicated, may hold values from 0 to 3, each once within a row
- params: float32 [2, 5120, 1024], P(None, 'fsdp', 'tp'), may hold values from -0.75 to 0.75
- moment1: float32 [2, 5120, 1024], P(None, 'fsdp', 'tp'), may hold values from -0.15625 to 0.15625
- moment2: float32 [2, 5120, 1024], P(None, 'fsdp', 'tp'), may hold values from 0.0001 to 0.004
Outputs:
- new_params: float32 [2, 5120, 1024], P(None, 'fsdp', 'tp')
- new_moment1: float32 [2, 5120, 1024], P(None, 'fsdp', 'tp')
- new_moment2: float32 [2, 5120, 1024], P(None, 'fsdp', 'tp')
- rollout_delta: bfloat16 [2, 5120, 1024], P(None, None, 'tp')
The draws below stay inside these ranges and needn't reach their ends.
Inputs may be any that keep to these rules, and one draw needn't show every extreme that they name: `owner_map`: each row is a permutation of 0 to 3.
All inputs are finite; a program needn't handle non-finite values.
Results may differ from the reference program's by a relative error of at most 0.0004.
Values may be sent and summed in bfloat16 or wider, within the bound.
No kernel may reach another device: no remote copies, remote signals or barrier semaphores. Data moves between devices by JAX's collectives and lax.ppermute only.
A program may use at most 64 MiB of HBM per device.

```python
import math
import jax
import jax.numpy as jnp
from jax import lax

D = 5120
KV = 1024
LAYERS = 2
STEP = 10
N_FSDP = 32
N_TP = 4


def draw_token_counts(key, part):
    base = jax.random.randint(key, (N_FSDP,), 100, 200)
    ramp = jnp.arange(N_FSDP, dtype=jnp.int32) * 400 // max(N_FSDP - 1, 1)
    position = jnp.arange(N_FSDP, dtype=jnp.int32)
    counts = jnp.where(position == 0, 100, base + ramp)
    counts = jnp.where(position == N_FSDP - 1, 599, counts)
    return counts.astype(jnp.int32)


def spiked(values, own_key, source, target, shards_of, factor):
    def block_of(dim):
        return (jnp.arange(values.shape[dim]) // (values.shape[dim] // shards_of)).reshape((-1,) + (1,) * (values.ndim - 1 - dim))

    near = jax.random.permutation(own_key, shards_of)[block_of(target)]
    far = (block_of(target) + shards_of // 2) % shards_of
    return jnp.where((block_of(source) == near) | (block_of(source) == far), factor * values, values)


def block_levels(key, shape, cuts, least, largest):
    loudness = 1.0
    for dim, blocks in cuts:
        draws = jax.random.uniform(jax.random.fold_in(jax.random.fold_in(key, 6), dim), (blocks,), jnp.float32, least / len(cuts), largest / len(cuts))
        loudness = loudness * jnp.repeat(jnp.exp(draws), shape[dim] // blocks).reshape((-1,) + (1,) * (len(shape) - 1 - dim))
    return loudness


def scatter_about(stream_key, dims, width, limit, pieces=(), held_as=jnp.bfloat16):
    drawn = jax.random.normal(stream_key, dims, jnp.float32) * width
    if len(pieces) > 0:
        drawn = block_levels(stream_key, dims, pieces, -0.22, 0.18) * drawn
    return jnp.clip(drawn, min=-limit, max=limit).astype(held_as)


def bell_draw_with(rng, extent, scale, reach, split, heavy, kind=jnp.bfloat16):
    drawn = scale * jax.random.normal(rng, extent, jnp.float32)
    if split:
        drawn = drawn * block_levels(rng, extent, split, -0.22, 0.18)
    return jnp.clip(spiked(drawn, jax.random.fold_in(rng, 3), *heavy), -reach, reach).astype(kind)


def setup_inputs(seed: int = 0) -> dict:
    streams_of = jax.random.split(jax.random.key(seed), 7)
    return {
        "partials": bell_draw_with(streams_of[0], (N_FSDP, LAYERS, D, KV), 1.0, 6.0, ((0, 32), (3, 4)), (0, 2, 32, 2.75)),
        "token_counts": draw_token_counts(jax.random.fold_in(streams_of[6], 71), 0),
        "owner_map": jax.vmap(lambda own: jax.random.permutation(own, N_TP))(jax.random.split(streams_of[2], LAYERS)).reshape((LAYERS, N_TP)).astype(jnp.int32),
        "params": scatter_about(streams_of[3], (LAYERS, D, KV), 0.05, 0.75, ((1, 32), (2, 4)), jnp.float32),
        "moment1": scatter_about(streams_of[4], (LAYERS, D, KV), 0.01, 0.15625, ((1, 32), (2, 4)), jnp.float32),
        "moment2": jnp.clip(jnp.exp(math.log(0.004) - 3.6888795 * jax.random.uniform(streams_of[5], (LAYERS, D, KV), jnp.float32) ** block_levels(streams_of[5], (LAYERS, D, KV), ((1, 32), (2, 4)), -0.2, 0.2)), 0.0001, 0.004),
    }


def reference(partials, token_counts, owner_map, params, moment1, moment2):
    weights = token_counts.astype(jnp.float32)
    total = jnp.sum(weights)

    def accumulate(summed, pair):
        term, weight = pair
        return (summed + weight * term.astype(jnp.float32), None)
    summed, _ = lax.scan(accumulate, jnp.zeros((LAYERS, D, KV), jnp.float32), (partials, weights))
    grad = summed / total
    first = 0.9 * moment1 + 0.1 * grad
    second = 0.999 * moment2 + 0.001 * grad * grad
    bias_one = 1.0 - 0.9 ** STEP
    bias_two = 1.0 - 0.999 ** STEP
    direction = first / bias_one / (jnp.sqrt(second / bias_two) + 1e-08)
    new_params = params - 0.001 * (direction + 0.1 * params)
    delta = direction.astype(jnp.bfloat16)
    blocks = delta.reshape(LAYERS, D, N_TP, KV // N_TP)
    chosen = owner_map.astype(jnp.int32)[:, None, :, None]
    rollout = jnp.take_along_axis(blocks, chosen, axis=2).reshape(LAYERS, D, KV)
    return (new_params, first, second, rollout)
```

```python
import jax
import jax.numpy as jnp
from jax import lax
from jax.experimental import pallas as pl
from jax.experimental.pallas import tpu as pltpu
from jax.sharding import Mesh
from jax.sharding import PartitionSpec as P

STEP = 10
FSDP = ("y", "zl", "x")


def ring(n, k):
    return [(i, (i + k) % n) for i in range(n)]


def along_z(flip_lo, flip_hi):
    pairs = []
    for lo in range(2):
        for hi in range(2):
            pairs.append((lo * 2 + hi, (lo ^ flip_lo) * 2 + (hi ^ flip_hi)))
    return pairs


def served_rows(delta, owner_map):
    core, z_hi, z_lo = lax.axis_index("core"), lax.axis_index("zh"), lax.axis_index("zl")
    other = lax.ppermute(delta, "core", [(0, 1), (1, 0)])
    even = jnp.where(core == 0, delta, other)
    odd = jnp.where(core == 0, other, delta)

    def block_for(hi):
        wanted = lax.dynamic_index_in_dim(owner_map, 2 * hi + core, 1, keepdims=False)
        picked = jnp.where((wanted % 2 == 1)[:, None, None], odd, even)
        return picked, (wanted // 2 == z_hi)[:, None, None]

    mine, here = block_for(z_hi)
    theirs, _ = block_for(1 - z_hi)
    beside = lax.ppermute(mine, ("zl", "zh"), along_z(1, 0))
    across = lax.ppermute(theirs, ("zl", "zh"), along_z(0, 1))
    corner = lax.ppermute(theirs, ("zl", "zh"), along_z(1, 1))
    own = jnp.where(here, mine, across)
    peer = jnp.where(here, beside, corner)
    low = jnp.where(z_lo == 0, own, peer)
    high = jnp.where(z_lo == 0, peer, own)
    return jnp.stack([low, high], 1)


def from_ring(value, axis):
    return [value] + [lax.ppermute(value, axis, ring(4, k)) for k in (1, 2, 3)]


def place(first, second, shape):
    rows, cols = shape

    def body(*refs):
        ins, out, sem = refs[:8], refs[8], refs[9]
        x, y = lax.axis_index("x"), lax.axis_index("y")
        copies = []
        for a in range(4):
            for b in range(4):
                copies.append(
                    pltpu.make_async_copy(
                        ins[a].at[b],
                        out.at[0, lax.rem(y + 4 - a, 4), :, lax.rem(x + 4 - b, 4)],
                        sem.at[len(copies)],
                    )
                )
                copies.append(
                    pltpu.make_async_copy(
                        ins[4 + a].at[b],
                        out.at[1, lax.rem(y + 4 - b, 4), :, lax.rem(x + 4 - a, 4)],
                        sem.at[len(copies)],
                    )
                )
        for copy in copies:
            copy.start()
        for copy in copies:
            copy.wait()

    return pl.pallas_call(
        body,
        out_shape=jax.ShapeDtypeStruct((2, 4, 2, 4, rows, cols), jnp.bfloat16),
        in_specs=[pl.BlockSpec(memory_space=pltpu.VMEM)] * 8,
        out_specs=pl.BlockSpec(memory_space=pl.ANY),
        scratch_shapes=[pltpu.SemaphoreType.DMA((32,))],
        compiler_params=pltpu.CompilerParams(vmem_limit_bytes=16 * 1024 * 1024),
        cost_estimate=pl.CostEstimate(flops=2**22, bytes_accessed=2**23, transcendentals=0),
    )(*first, *second)


def local(partials, token_counts, owner_map, params, moment1, moment2):
    layers, rows, cols = params.shape
    count = token_counts[0]
    coarse = (count // 8 * 8).astype(jnp.bfloat16)
    fine = (count % 8).astype(jnp.bfloat16)
    tag = jnp.where(lax.broadcasted_iota(jnp.int32, (32, 8, cols), 2) < cols // 2, coarse, fine)
    terms = partials.reshape(layers, 32, rows, cols).transpose(1, 0, 2, 3)
    packed = jnp.concatenate([terms.reshape(32, layers * rows, cols), tag], 1)
    arrived = lax.all_to_all(packed, FSDP, split_axis=0, concat_axis=0, tiled=True)
    marks = arrived[:, layers * rows, :].astype(jnp.float32)
    counts = marks[:, 0] + marks[:, cols // 2]
    total = jnp.sum(counts)
    body = arrived[:, : layers * rows].reshape(32, layers, rows, cols)
    summed = jnp.sum(counts[:, None, None, None] * body.astype(jnp.float32), axis=0)
    grad = summed / total
    first = 0.9 * moment1 + 0.1 * grad
    second = 0.999 * moment2 + 0.001 * grad * grad
    bias_one = 1.0 - 0.9**STEP
    bias_two = 1.0 - 0.999**STEP
    direction = first / bias_one / (jnp.sqrt(second / bias_two) + 1e-08)
    new_params = params - 0.001 * (direction + 0.1 * params)
    delta = direction.astype(jnp.bfloat16)
    served = served_rows(delta, owner_map)
    by_x = jnp.stack(from_ring(served[0], "x"))
    by_y = jnp.stack(from_ring(served[1], "y"))
    rollout = place(from_ring(by_x, "y"), from_ring(by_y, "x"), (rows, cols))
    return (new_params, first, second, rollout.reshape(layers, 32 * rows, cols))


def solution(mesh):
    split = Mesh(mesh.devices.reshape(4, 2, 4, 2, 2), ("y", "zl", "x", "zh", "core"))
    tp = ("zh", "core")
    state = P(None, FSDP, tp)
    return jax.shard_map(
        local,
        mesh=split,
        in_specs=(P(FSDP, None, None, tp), P(FSDP), P(), state, state, state),
        out_specs=(state, state, state, P(None, None, tp)),
        check_vma=False,
    )
```

```python
import jax
import jax.numpy as jnp
from jax import lax
from jax.experimental import pallas as pl
from jax.experimental.pallas import tpu as pltpu
from jax.sharding import Mesh
from jax.sharding import PartitionSpec as P

STEP = 10
FSDP = ("y", "zl", "x")
VMEM = pl.BlockSpec(memory_space=pltpu.VMEM)
HBM = pl.BlockSpec(memory_space=pltpu.HBM)
SMEM = pl.BlockSpec(memory_space=pltpu.SMEM)
ROWS, COLS = 160, 256
SIZE = 8 * ROWS
GROUPS = ((1, 3), (2, 0))
BF16, F32 = jnp.bfloat16, jnp.float32


def step_to(k):
    return [(i, i ^ k) for i in range(4)]


def along_z(flip_lo, flip_hi):
    pairs = []
    for lo in range(2):
        for hi in range(2):
            pairs.append((lo * 2 + hi, (lo ^ flip_lo) * 2 + (hi ^ flip_hi)))
    return pairs


def kernel(body, outs, ins, args, scratch=(), work=2**20, spec=VMEM, aliases=None):
    return pl.pallas_call(
        body,
        out_shape=[jax.ShapeDtypeStruct(shape, dtype) for shape, dtype in outs],
        in_specs=ins,
        out_specs=[spec] * len(outs),
        scratch_shapes=list(scratch),
        input_output_aliases=aliases or {},
        compiler_params=pltpu.CompilerParams(vmem_limit_bytes=24 * 2**20),
        cost_estimate=pl.CostEstimate(flops=work, bytes_accessed=work, transcendentals=0),
    )(*args)


def places():
    return lax.axis_index("x"), lax.axis_index("y")


def blocks_for(cube, count, ks):
    def body(cube_ref, count_ref, *refs):
        outs, sem = refs[:-1], refs[-1]
        x, y = places()
        lo = lax.axis_index("zl")
        copies = []
        for n, k in enumerate(ks):
            for half in range(2):
                out, to = outs[2 * n + half], (y if half else x) ^ k
                for part, z in enumerate((1 - lo, lo)):
                    for i in range(4):
                        src = cube_ref.at[1, to, z, i] if half else cube_ref.at[0, i, z, to]
                        dst = out.at[pl.ds((4 * part + i) * ROWS, ROWS)]
                        copies.append(pltpu.make_async_copy(src, dst, sem.at[len(copies)]))
        for copy in copies:
            copy.start()
        value = count_ref[0]
        coarse = lax.div(value, 8) * 8
        row = lax.broadcasted_iota(jnp.int32, (16, COLS), 0)
        tag = jnp.where(row < 8, coarse, value - coarse).astype(F32).astype(BF16)
        for out in outs:
            out[pl.ds(SIZE, 16), :] = tag
        for copy in copies:
            copy.wait()

    return kernel(
        body,
        [((SIZE + 16, COLS), BF16)] * (2 * len(ks)),
        [HBM, SMEM],
        [cube, count],
        scratch=[pltpu.SemaphoreType.DMA((16 * len(ks),))],
    )


def weighted(blocks):
    def body(*refs):
        ins, outs, table = refs[:8], refs[8:16], refs[16]
        for k in range(8):
            tag = ins[k][pl.ds(SIZE, 16), :].astype(F32)
            table[pl.ds(k, 1), :] = tag[0:1] + tag[8:9]
        x, y = places()
        for half in range(2):
            scale = [table[pl.ds(4 * half + i, 1), :] for i in range(4)]
            for part in range(2):
                for k in range(4):
                    base = (((x if half else y) ^ k) + 4 * part) * ROWS
                    out = outs[4 * half + k]

                    def step(i, carry, base=base, out=out, half=half, part=part, scale=scale):
                        at = pl.multiple_of(base + i * 32, 32)
                        total = scale[0] * ins[4 * half][pl.ds(at, 32), :].astype(F32)
                        for j in (1, 2, 3):
                            total += scale[j] * ins[4 * half + j][pl.ds(at, 32), :].astype(F32)
                        out[pl.ds(pl.multiple_of(part * ROWS + i * 32, 32), 32), :] = total
                        return carry

                    lax.fori_loop(0, ROWS // 32, step, 0)
        mark = jnp.broadcast_to(table[0:1, :] + table[1:2, :] + table[2:3, :] + table[3:4, :], (8, COLS))
        for k in range(4):
            outs[k][pl.ds(2 * ROWS, 8), :] = mark

    outs = [((2 * ROWS + 8, COLS), F32)] * 4 + [((2 * ROWS, COLS), F32)] * 4
    return kernel(body, outs, [VMEM] * 8, blocks, scratch=[pltpu.VMEM((8, COLS), F32)], work=2**24)


def added(parts):
    def body(*refs):
        ins, outs = refs[:8], refs[8:]
        for half in range(2):
            for part in range(2):

                def step(i, carry, half=half, part=part):
                    at = pl.multiple_of(part * ROWS + i * 32, 32)
                    total = ins[4 * half][pl.ds(at, 32), :]
                    for j in (1, 2, 3):
                        total += ins[4 * half + j][pl.ds(at, 32), :]
                    outs[part][pl.ds(pl.multiple_of(half * ROWS + i * 32, 32), 32), :] = total
                    return carry

                lax.fori_loop(0, ROWS // 32, step, 0)
        tail = pl.ds(2 * ROWS, 8)
        outs[0][tail, :] = ins[0][tail, :] + ins[1][tail, :] + ins[2][tail, :] + ins[3][tail, :]

    outs = [((2 * ROWS + 8, COLS), F32), ((2 * ROWS, COLS), F32)]
    return kernel(body, outs, [VMEM] * 8, parts, work=2**20)


def reduced(partials, token_counts):
    cube = pltpu.with_memory_space_constraint(partials.reshape(2, 4, 2, 4, ROWS, COLS), pltpu.HBM)
    got = {}
    for ks in GROUPS:
        made = blocks_for(cube, token_counts, ks)
        for n, k in enumerate(ks):
            for half, axis in enumerate(("x", "y")):
                block = made[2 * n + half]
                got[half, k] = lax.ppermute(block, axis, step_to(k)) if k else block
    sums = list(weighted([got[half, k] for half in range(2) for k in range(4)]))
    for k in (1, 3, 2):
        for half, axis in enumerate(("y", "x")):
            sums[4 * half + k] = lax.ppermute(sums[4 * half + k], axis, step_to(k))
    send, kept = added(sums)
    peer = lax.ppermute(send, "zl", [(0, 1), (1, 0)])
    total = send[-1:] + peer[-1:]
    return (kept + peer[: 2 * ROWS]).reshape(2, ROWS, COLS), total[None]


def served_rows(delta, owner_map):
    core, z_hi, z_lo = lax.axis_index("core"), lax.axis_index("zh"), lax.axis_index("zl")
    other = lax.ppermute(delta, "core", [(0, 1), (1, 0)])
    even = jnp.where(core == 0, delta, other)
    odd = jnp.where(core == 0, other, delta)

    def block_for(hi):
        wanted = lax.dynamic_index_in_dim(owner_map, 2 * hi + core, 1, keepdims=False)
        picked = jnp.where((wanted % 2 == 1)[:, None, None], odd, even)
        return picked, (wanted // 2 == z_hi)[:, None, None]

    mine, here = block_for(z_hi)
    theirs, _ = block_for(1 - z_hi)
    beside = lax.ppermute(mine, ("zl", "zh"), along_z(1, 0))
    across = lax.ppermute(theirs, ("zl", "zh"), along_z(0, 1))
    corner = lax.ppermute(theirs, ("zl", "zh"), along_z(1, 1))
    own = jnp.where(here, mine, across)
    peer = jnp.where(here, beside, corner)
    low = jnp.where(z_lo == 0, own, peer)
    high = jnp.where(z_lo == 0, peer, own)
    return jnp.stack([low, high], 1)


def place(out, pieces):
    held = [] if out is None else [out]

    def body(*refs):
        ins, dst, sem = refs[len(held) : -2], refs[-2], refs[-1]
        x, y = places()
        copies = []
        for ref, (layer, a, bs, _) in zip(ins, pieces):
            for n, b in enumerate(bs):
                to = dst.at[1, y ^ b, :, x ^ a] if layer else dst.at[0, y ^ a, :, x ^ b]
                copies.append(pltpu.make_async_copy(ref.at[n], to, sem.at[len(copies)]))
        for copy in copies:
            copy.start()
        for copy in copies:
            copy.wait()

    return kernel(
        body,
        [((2, 4, 2, 4, ROWS, COLS), BF16)],
        [HBM] * len(held) + [VMEM] * len(pieces),
        held + [piece[3] for piece in pieces],
        scratch=[pltpu.SemaphoreType.DMA((sum(len(piece[2]) for piece in pieces),))],
        work=2**22,
        spec=HBM,
        aliases={0: 0} if held else None,
    )[0]


def gathered(served):
    near = []
    for layer, axis in enumerate(("x", "y")):
        near.append([served[layer]] + [lax.ppermute(served[layer], axis, step_to(k)) for k in (1, 2, 3)])
    near = lax.optimization_barrier(near)
    early, late = [], []
    for layer, axis in enumerate(("y", "x")):
        head, tail = jnp.stack(near[layer][:2]), jnp.stack(near[layer][2:])
        early += [(layer, 0, (0, 1), head), (layer, 0, (2, 3), tail)]
        head_one, tail_three = lax.ppermute(head, axis, step_to(1)), lax.ppermute(tail, axis, step_to(3))
        tail_one, head_three = lax.ppermute(tail, axis, step_to(1)), lax.ppermute(head, axis, step_to(3))
        early += [(layer, 1, (0, 1), head_one), (layer, 1, (2, 3), tail_one)]
        early += [(layer, 3, (0, 1), head_three), (layer, 3, (2, 3), tail_three)]
        late += [(layer, 2, (0, 1), lax.ppermute(head_one, axis, step_to(3)))]
        late += [(layer, 2, (2, 3), lax.ppermute(tail_three, axis, step_to(1)))]
    return place(place(None, early), late)


def local(partials, token_counts, owner_map, params, moment1, moment2):
    summed, total = reduced(partials[0], token_counts)
    grad = summed / total
    first = 0.9 * moment1 + 0.1 * grad
    second = 0.999 * moment2 + 0.001 * grad * grad
    bias_one = 1.0 - 0.9**STEP
    bias_two = 1.0 - 0.999**STEP
    direction = first / bias_one / (jnp.sqrt(second / bias_two) + 1e-08)
    new_params = params - 0.001 * (direction + 0.1 * params)
    rollout = gathered(served_rows(direction.astype(BF16), owner_map))
    return (new_params, first, second, rollout.reshape(2, 32 * ROWS, COLS))


def solution(mesh):
    split = Mesh(mesh.devices.reshape(4, 2, 4, 2, 2), ("y", "zl", "x", "zh", "core"))
    tp = ("zh", "core")
    state = P(None, FSDP, tp)
    return jax.shard_map(
        local,
        mesh=split,
        in_specs=(P(FSDP, None, None, tp), P(FSDP), P(), state, state, state),
        out_specs=(state, state, state, P(None, None, tp)),
        check_vma=False,
    )
```

```python
import jax
import jax.numpy as jnp
from jax import lax
from jax.experimental import pallas as pl
from jax.experimental.pallas import tpu as pltpu
from jax.sharding import Mesh
from jax.sharding import PartitionSpec as P

STEP = 10
FSDP = ("y", "zl", "x")
VMEM = pl.BlockSpec(memory_space=pltpu.VMEM)
HBM = pl.BlockSpec(memory_space=pltpu.HBM)
SMEM = pl.BlockSpec(memory_space=pltpu.SMEM)
ROWS, COLS = 160, 256
SIZE = 4 * ROWS
GROUPS = {"a": ((1, 3, 2), (0,)), "h": ((1, 3, 2, 0),)}
BF16, F32 = jnp.bfloat16, jnp.float32


def sent(value, axis, k):
    return lax.ppermute(value, axis, step_to(k))


def step_to(k):
    return [(i, i ^ k) for i in range(4)]


def along_z(flip_lo, flip_hi):
    pairs = []
    for lo in range(2):
        for hi in range(2):
            pairs.append((lo * 2 + hi, (lo ^ flip_lo) * 2 + (hi ^ flip_hi)))
    return pairs


def kernel(body, outs, ins, args, scratch=(), work=2**20, spec=VMEM, aliases=None):
    return pl.pallas_call(
        body,
        out_shape=[jax.ShapeDtypeStruct(shape, dtype) for shape, dtype in outs],
        in_specs=ins,
        out_specs=[spec] * len(outs),
        scratch_shapes=list(scratch),
        input_output_aliases=aliases or {},
        compiler_params=pltpu.CompilerParams(vmem_limit_bytes=8 * 2**20),
        cost_estimate=pl.CostEstimate(flops=work, bytes_accessed=work, transcendentals=0),
    )(*args)


def places():
    return lax.axis_index("x"), lax.axis_index("y")


def blocks_for(cube, count, ks, tagged):
    def body(cube_ref, count_ref, *refs):
        outs, sem = refs[:-1], refs[-1]
        x, y = places()
        lo = lax.axis_index("zl")
        z = 1 - lo if tagged else lo
        copies = []
        for n, k in enumerate(ks):
            for half in range(2):
                out, to = outs[2 * n + half], (y if half else x) ^ k
                for i in range(4):
                    src = cube_ref.at[1, to, z, i] if half else cube_ref.at[0, i, z, to]
                    dst = out.at[pl.ds(i * ROWS, ROWS)]
                    copies.append(pltpu.make_async_copy(src, dst, sem.at[len(copies)]))
        for copy in copies:
            copy.start()
        if tagged:
            value = count_ref[0]
            coarse = lax.div(value, 8) * 8
            row = lax.broadcasted_iota(jnp.int32, (16, COLS), 0)
            tag = jnp.where(row < 8, coarse, value - coarse).astype(F32).astype(BF16)
            for out in outs:
                out[pl.ds(SIZE, 16), :] = tag
        for copy in copies:
            copy.wait()

    return kernel(
        body,
        [((SIZE + (16 if tagged else 0), COLS), BF16)] * (2 * len(ks)),
        [HBM, SMEM],
        [cube, count],
        scratch=[pltpu.SemaphoreType.DMA((8 * len(ks),))],
    )


def weighted(blocks, weights=None):
    tagged = weights is None

    def body(*refs):
        ins = refs[:8]
        if tagged:
            outs, table = refs[8:16], refs[16]
            for k in range(8):
                tag = ins[k][pl.ds(SIZE, 16), :].astype(F32)
                table[pl.ds(k, 1), :] = tag[0:1] + tag[8:9]
        else:
            table, outs = refs[8], refs[9:17]
        x, y = places()
        for half in range(2):
            scale = [table[pl.ds(4 * half + i, 1), :] for i in range(4)]
            for k in range(4):
                base = ((x if half else y) ^ k) * ROWS
                out = outs[4 * half + k]

                def step(i, carry, base=base, out=out, half=half, scale=scale):
                    at = pl.multiple_of(base + i * 32, 32)
                    total = scale[0] * ins[4 * half][pl.ds(at, 32), :].astype(F32)
                    for j in (1, 2, 3):
                        total += scale[j] * ins[4 * half + j][pl.ds(at, 32), :].astype(F32)
                    out[pl.ds(pl.multiple_of(i * 32, 32), 32), :] = total
                    return carry

                lax.fori_loop(0, ROWS // 32, step, 0)
        if tagged:
            mark = jnp.broadcast_to(table[0:1, :] + table[1:2, :] + table[2:3, :] + table[3:4, :], (8, COLS))
            for k in range(4):
                outs[k][pl.ds(ROWS, 8), :] = mark

    outs = [((ROWS + (8 if tagged else 0), COLS), F32)] * 4 + [((ROWS, COLS), F32)] * 4
    if tagged:
        return kernel(body, outs + [((8, COLS), F32)], [VMEM] * 8, blocks, work=2**24)
    return kernel(body, outs, [VMEM] * 9, [*blocks, weights], work=2**24)


def added(parts, halves=None):
    def body(*refs):
        ins, refs = refs[:8], refs[8:]
        sides, outs = (refs[:2], refs[2:]) if halves else ((), refs)
        for half in range(2):

            def step(i, carry, half=half):
                at = pl.multiple_of(i * 32, 32)
                to = pl.ds(pl.multiple_of(half * ROWS + i * 32, 32), 32)
                total = ins[4 * half][pl.ds(at, 32), :]
                for j in (1, 2, 3):
                    total += ins[4 * half + j][pl.ds(at, 32), :]
                if halves:
                    total += sides[1][to, :]
                outs[0][to, :] = total
                return carry

            lax.fori_loop(0, ROWS // 32, step, 0)
        end = pl.ds(2 * ROWS, 8)
        if halves:
            outs[1][...] = sides[0][end, :] + sides[1][end, :]
        else:
            tail = pl.ds(ROWS, 8)
            outs[0][end, :] = ins[0][tail, :] + ins[1][tail, :] + ins[2][tail, :] + ins[3][tail, :]

    if halves:
        outs = [((2 * ROWS, COLS), F32), ((8, COLS), F32)]
        return kernel(body, outs, [VMEM] * 10, [*parts, *halves], work=2**20)
    return kernel(body, [((2 * ROWS + 8, COLS), F32)], [VMEM] * 8, parts, work=2**20)[0]


def fetched(*arrays):
    def body(*refs):
        copies = [pltpu.make_async_copy(refs[i], refs[2 + i], refs[4].at[i]) for i in range(2)]
        for copy in copies:
            copy.start()
        for copy in copies:
            copy.wait()

    args = [pltpu.with_memory_space_constraint(array, pltpu.HBM) for array in arrays]
    outs = [(array.shape, array.dtype) for array in arrays]
    return kernel(body, outs, [HBM] * 2, args, scratch=[pltpu.SemaphoreType.DMA((2,))])


def reduced(partials, token_counts):
    cube = pltpu.with_memory_space_constraint(partials.reshape(2, 4, 2, 4, ROWS, COLS), pltpu.HBM)
    weights = None
    for part, tagged in (("a", True), ("h", False)):
        got = {}
        for n, ks in enumerate(GROUPS[part]):
            made = blocks_for(cube, token_counts, ks, tagged)
            for n, k in enumerate(ks):
                for half, axis in enumerate(("x", "y")):
                    block = made[2 * n + half]
                    got[half, k] = sent(block, axis, k) if k else block
        sums = list(weighted([got[half, k] for half in range(2) for k in range(4)], weights))
        if tagged:
            weights = sums.pop()
        for k in (1, 3, 2):
            for half, axis in enumerate(("y", "x")):
                sums[4 * half + k] = sent(sums[4 * half + k], axis, k)
        if tagged:
            send = added(sums)
            peer = lax.ppermute(send, "zl", [(0, 1), (1, 0)])
        else:
            summed, total = added(sums, (send, peer))
    return summed.reshape(2, ROWS, COLS), total[:1][None]


def served_rows(delta, owner_map):
    core, z_hi, z_lo = lax.axis_index("core"), lax.axis_index("zh"), lax.axis_index("zl")
    other = lax.ppermute(delta, "core", [(0, 1), (1, 0)])
    even = jnp.where(core == 0, delta, other)
    odd = jnp.where(core == 0, other, delta)

    def block_for(hi):
        wanted = lax.dynamic_index_in_dim(owner_map, 2 * hi + core, 1, keepdims=False)
        picked = jnp.where((wanted % 2 == 1)[:, None, None], odd, even)
        return picked, (wanted // 2 == z_hi)[:, None, None]

    mine, here = block_for(z_hi)
    theirs, _ = block_for(1 - z_hi)
    beside = lax.ppermute(mine, ("zl", "zh"), along_z(1, 0))
    across = lax.ppermute(theirs, ("zl", "zh"), along_z(0, 1))
    corner = lax.ppermute(theirs, ("zl", "zh"), along_z(1, 1))
    own = jnp.where(here, mine, across)
    peer = jnp.where(here, beside, corner)
    low = jnp.where(z_lo == 0, own, peer)
    high = jnp.where(z_lo == 0, peer, own)
    return jnp.stack([low, high], 1)


def place(out, pieces):
    held = [] if out is None else [out]

    def body(*refs):
        ins, dst, sem = refs[len(held) : -2], refs[-2], refs[-1]
        x, y = places()
        copies = []
        for ref, (layer, a, bs, _) in zip(ins, pieces):
            for n, b in enumerate(bs):
                to = dst.at[1, y ^ b, :, x ^ a] if layer else dst.at[0, y ^ a, :, x ^ b]
                copies.append(pltpu.make_async_copy(ref.at[n], to, sem.at[len(copies)]))
        for copy in copies:
            copy.start()
        for copy in copies:
            copy.wait()

    return kernel(
        body,
        [((2, 4, 2, 4, ROWS, COLS), BF16)],
        [HBM] * len(held) + [VMEM] * len(pieces),
        held + [piece[3] for piece in pieces],
        scratch=[pltpu.SemaphoreType.DMA((sum(len(piece[2]) for piece in pieces),))],
        work=2**22,
        spec=HBM,
        aliases={0: 0} if held else None,
    )[0]


def gathered(served):
    near = []
    for layer, axis in enumerate(("x", "y")):
        near.append([served[layer]] + [sent(served[layer], axis, k) for k in (1, 2, 3)])
    own, early, late = [], [], []
    for layer, axis in enumerate(("y", "x")):
        head, tail = jnp.stack(near[layer][:2]), jnp.stack(near[layer][2:])
        own += [(layer, 0, (0, 1), head), (layer, 0, (2, 3), tail)]
        head_one, tail_three = sent(head, axis, 1), sent(tail, axis, 3)
        tail_one, head_three = sent(tail, axis, 1), sent(head, axis, 3)
        own += [(layer, 1, (0, 1), head_one), (layer, 3, (2, 3), tail_three)]
        early += [(layer, 1, (2, 3), tail_one), (layer, 3, (0, 1), head_three)]
        late += [(layer, 2, (0, 1), sent(head_one, axis, 3))]
        late += [(layer, 2, (2, 3), sent(tail_three, axis, 1))]
    return place(place(place(None, own), early), late)


def update(partials, token_counts, owner_map, params, moment1, moment2):
    near = fetched(moment1, moment2)
    summed, total = reduced(partials[0], token_counts)
    moment1, moment2 = near
    grad = summed / total
    first = 0.9 * moment1 + 0.1 * grad
    second = 0.999 * moment2 + 0.001 * grad * grad
    bias_one = 1.0 - 0.9**STEP
    bias_two = 1.0 - 0.999**STEP
    direction = first / bias_one / (jnp.sqrt(second / bias_two) + 1e-08)
    new_params = params - 0.001 * (direction + 0.1 * params)
    rollout = gathered(served_rows(direction.astype(BF16), owner_map))
    return (new_params, first, second, rollout.reshape(2, 32 * ROWS, COLS))


def solution(mesh):
    split = Mesh(mesh.devices.reshape(4, 2, 4, 2, 2), ("y", "zl", "x", "zh", "core"))
    tp = ("zh", "core")
    state = P(None, FSDP, tp)
    return jax.shard_map(
        update,
        mesh=split,
        in_specs=(P(FSDP, None, None, tp), P(FSDP), P(), state, state, state),
        out_specs=(state, state, state, P(None, None, tp)),
        check_vma=False,
    )
```
